32 devices in a mesh: ep: 16 (over z, y, x), tp: 2 (over core).
Axes of the slice: x: 2, y: 2, z: 4, core: 2. Of those that a mesh axis runs over, the one named last changes fastest.
Arguments:
- tokens: bfloat16 [2048, 3584], P('ep', 'tp'), may hold values from -6 to 6
- routes: int32 [2048, 8], P('ep'), may hold values from 0 to 15, all different within a row; in each aligned block of 128 rows (0 to 127, 128 to 255, ...) at most 72 rows name the same one
- gate_levels: int32 [2048, 8], P('ep'), may hold values from 1 to 255
- w_gate: bfloat16 [16, 3584, 1024], P('ep', 'tp'), may hold values from -0.09375 to 0.09375
- w_up: bfloat16 [16, 3584, 1024], P('ep', 'tp'), may hold values from -0.09375 to 0.09375
- w_down: bfloat16 [16, 1024, 3584], P('ep', None, 'tp'), may hold values from -0.1875 to 0.1875
Outputs:
- mixed: bfloat16 [2048, 3584], P('ep', 'tp')
The draws below stay inside these ranges and needn't reach their ends.
Inputs may be any that keep to these rules, and one draw needn't show every extreme that they name: `routes`: each row names 8 different experts. Among the 128 tokens of one aligned block no expert is named by more than 72 rows, and in every draw some expert is named by exactly 72 rows of some block.
All inputs are finite; a program needn't handle non-finite values.
Results may differ from the reference program's by a relative error of at most 0.0085.
Values may be sent and summed in bfloat16 or wider, within the bound.
No kernel may reach another device: no remote copies, remote signals or barrier semaphores. Data moves between devices by JAX's collectives and lax.ppermute only.
A program may use at most 64 MiB of HBM per device.

```python
import math
import jax
import jax.numpy as jnp
import numpy as np
from jax import lax

D = 3584
FF = 1024
TOP = 8
TOK_EP = 128
EXPERTS = 16
CAP = 72
TOKENS = 2048
N_EP = 16


def plant(values, rng, least, largest):
    index_at = [jax.random.randint(jax.random.fold_in(rng, axis), (), 0, length) for axis, length in enumerate(values.shape)]
    main_axis = values.shape.index(max(values.shape))
    beside = index_at[:main_axis] + [(index_at[main_axis] + 1) % values.shape[main_axis]] + index_at[main_axis + 1:]
    return values.at[tuple(index_at)].set(least).at[tuple(beside)].set(largest)


def level_of(stream_key, extent, pieces, least, high):
    gain = 1.0
    for position, parts in pieces:
        draws = jax.random.uniform(jax.random.fold_in(jax.random.fold_in(stream_key, 6), position), (parts,), jnp.float32, least / len(pieces), high / len(pieces))
        gain = gain * jnp.repeat(jnp.exp(draws), extent[position] // parts).reshape((-1,) + (1,) * (len(extent) - 1 - position))
    return gain


def deal_out(rng, own, number, rows, count, top, bound, slope):
    order = jax.random.permutation(rng, count)
    packed, common = portions_of(count, rows * top, bound, slope, True), portions_of(count, rows * top, bound, slope, False)
    places = jnp.arange(count)

    def named(tallies, rotation):
        used = int((tallies > 0).sum())
        fixed = max(1, used // 4)
        passed = fixed + (places - fixed + rotation * (used - fixed)) % max(1, count - fixed)
        return jnp.zeros((count,), jnp.int32).at[order[jnp.where(places < fixed, places, passed)]].set(jnp.asarray(tallies, jnp.int32))

    tallies = jnp.where(number % 4 == 0, named(packed, number // 4), named(common, number - number // 4 - 1))
    mixed = jax.random.permutation(jax.random.fold_in(own, 3), count)
    giver, taker = mixed[0:count // 2 * 2:2], mixed[1:count // 2 * 2:2]
    room = jnp.minimum(tallies[giver] - 1, bound - tallies[taker]) // 2
    room = jnp.where((giver == order[0]) | (taker == order[0]) | (tallies[taker] == 0), 0, jnp.maximum(room, 0))
    passed = jax.random.randint(jax.random.fold_in(own, 4), (count // 2,), 0, 1 << 20) % (room + 1)
    tallies = tallies.at[giver].add(-passed).at[taker].add(passed)
    labels = jnp.searchsorted(jnp.cumsum(tallies), jnp.arange(rows * top), side="right").astype(jnp.int32)
    listing = labels.reshape(top, rows).T
    listing = listing[jax.random.permutation(jax.random.fold_in(own, 1), rows)]
    rotation = jax.random.randint(jax.random.fold_in(own, 2), (rows, 1), 0, top)
    return jnp.take_along_axis(listing, (jnp.arange(top)[None, :] + rotation) % top, axis=1)


def portions_of(count, total, limit, skew, full):
    portions = [(1 << 20) // math.isqrt(grade ** skew) + 1 for grade in range(1, count + 1)]
    largest = limit if full else min(limit, max(-(-total // count), total * portions[0] // sum(portions)))
    least = 1 if total - largest >= count - 1 else 0
    counts, rest = [largest] + [least] * (count - 1), total - largest - least * (count - 1)
    while rest > 0:
        movable = [i for i in range(1, count) if counts[i] < largest] or [i for i in range(1, count) if counts[i] < limit]
        mass, left = sum([portions[i] for i in movable]), rest
        for i in movable:
            more = min(limit - counts[i], max(1, left * portions[i] // mass), rest)
            counts[i] = counts[i] + more
            rest = rest - more
    return np.array(counts)


def gaussian(key, extent, deviation, reach, cuts=(), kind=jnp.bfloat16):
    loudness = level_of(key, extent, cuts, -0.22, 0.18) if cuts else 1.0
    entries = jax.random.normal(key, extent, jnp.float32) * deviation * loudness
    return jnp.minimum(jnp.maximum(entries, -reach), reach).astype(kind)


def setup_inputs(seed: int = 0) -> dict:
    arg_keys = jax.random.split(jax.random.key(seed), 7)
    tokens = gaussian(arg_keys[0], (TOKENS, D), 1.0, 6.0, ((0, 16), (1, 2)))
    routes_keys = jax.random.split(jax.random.fold_in(arg_keys[1], 1), TOKENS // TOK_EP)
    routes_turns = jax.random.permutation(jax.random.fold_in(arg_keys[1], 3), TOKENS // TOK_EP)
    routes = jax.vmap(lambda own, number: deal_out(jax.random.fold_in(arg_keys[1], 2), own, number, TOK_EP, EXPERTS, TOP, CAP, 2))(routes_keys, routes_turns).reshape((TOKENS, TOP))
    gate_levels = plant(jax.random.randint(arg_keys[2], (TOKENS, TOP), 1, 256), jax.random.fold_in(arg_keys[2], 1), 1, 255).astype(jnp.int32)
    w_gate = gaussian(arg_keys[3], (EXPERTS, D, FF), D ** -0.5, 0.09375, ((0, 16), (1, 2)))
    w_up = gaussian(arg_keys[4], (EXPERTS, D, FF), D ** -0.5, 0.09375, ((0, 16), (1, 2)))
    w_down = gaussian(arg_keys[5], (EXPERTS, FF, D), FF ** -0.5, 0.1875, ((0, 16), (2, 2)))
    return {"tokens": tokens, "routes": routes, "gate_levels": gate_levels, "w_gate": w_gate, "w_up": w_up, "w_down": w_down}


def expert_apply(operands):
    inputs, gate_w, up_w, down_w = operands
    gate_act = jnp.dot(inputs, gate_w, preferred_element_type=jnp.float32)
    up_act = jnp.dot(inputs, up_w, preferred_element_type=jnp.float32)
    hidden = (jax.nn.silu(gate_act) * up_act).astype(jnp.bfloat16)
    return jnp.dot(hidden, down_w, preferred_element_type=jnp.float32).astype(jnp.bfloat16)


def reference(tokens, routes, gate_levels, w_gate, w_up, w_down):
    block_rows = TOK_EP * TOP
    flat_ids = routes.reshape(N_EP, block_rows).astype(jnp.int32)
    same_expert = flat_ids[:, :, None] == flat_ids[:, None, :]
    positions = jnp.arange(block_rows, dtype=jnp.int32)
    earlier = positions[:, None] > positions[None, :]
    slot_index = jnp.sum(same_expert & earlier[None], axis=2).astype(jnp.int32)
    block_ids = jnp.arange(N_EP, dtype=jnp.int32)[:, None]
    buffer_index = (flat_ids * (N_EP * CAP) + block_ids * CAP + slot_index).reshape(-1).astype(jnp.int32)
    owners = (jnp.arange(TOKENS * TOP, dtype=jnp.int32) // TOP).astype(jnp.int32)
    expert_rows = jnp.zeros((EXPERTS * N_EP * CAP, D), jnp.bfloat16).at[buffer_index].set(tokens[owners])
    expert_rows = expert_rows.reshape(EXPERTS, N_EP * CAP, D)
    expert_out = lax.map(expert_apply, (expert_rows, w_gate, w_up, w_down))
    picked = expert_out.reshape(EXPERTS * N_EP * CAP, D)[buffer_index].reshape(TOKENS, TOP, D).astype(jnp.float32)
    levels = gate_levels.astype(jnp.float32)
    weights = levels / jnp.sum(levels, axis=1, keepdims=True)
    return jnp.sum(weights[:, :, None] * picked, axis=1).astype(jnp.bfloat16)
```

```python
import jax
import jax.numpy as jnp
from jax import lax
from jax.sharding import PartitionSpec as P

F32 = jnp.float32
BF16 = jnp.bfloat16
LANES = 128


def inner_size(count):
    size = 1
    while size * size < count and count % (2 * size) == 0:
        size *= 2
    return size


def swap_sum(own, other):
    if lax.axis_size("tp") == 2:
        return own + lax.ppermute(other.astype(BF16), "tp", [(0, 1), (1, 0)]).astype(F32)
    return own


def expert(rows, w_gate, w_up, w_down):
    gate_part = jnp.dot(rows, w_gate, preferred_element_type=F32)
    up_part = jnp.dot(rows, w_up, preferred_element_type=F32)
    ff = w_gate.shape[1]
    if lax.axis_size("tp") == 2:
        half = ff // 2
        first = lax.axis_index("tp") == 0
        keep = lambda part: jnp.where(first, part[:, :half], part[:, half:])
        give = lambda part: jnp.where(first, part[:, half:], part[:, :half]).astype(BF16)
        pairs = [(0, 1), (1, 0)]
        got = lax.ppermute(jnp.concatenate([give(gate_part), give(up_part)], axis=1), "tp", pairs)
        gate_sum = keep(gate_part) + got[:, :half].astype(F32)
        up_sum = keep(up_part) + got[:, half:].astype(F32)
        hidden = (jax.nn.silu(gate_sum) * up_sum).astype(BF16)
        other = lax.ppermute(hidden, "tp", pairs)
        hidden = jnp.concatenate(
            [jnp.where(first, hidden, other), jnp.where(first, other, hidden)], axis=1
        )
    else:
        gate_sum = lax.psum_scatter(gate_part, "tp", scatter_dimension=1, tiled=True)
        up_sum = lax.psum_scatter(up_part, "tp", scatter_dimension=1, tiled=True)
        hidden = (jax.nn.silu(gate_sum) * up_sum).astype(BF16)
        hidden = lax.all_gather(hidden, "tp", axis=1, tiled=True)
    return jnp.dot(hidden, w_down, preferred_element_type=F32).astype(BF16)


def on_device(tokens, routes, gate_levels, w_gate, w_up, w_down):
    ep_count = lax.axis_size("ep")
    tok_rows, top_count = routes.shape
    assert w_gate.shape[0] == 1
    capacity = min(tok_rows, max(2, 9 * tok_rows * top_count // (8 * ep_count)))
    width = tokens.shape[1]
    inner = inner_size(ep_count)
    outer = ep_count // inner
    plane = lax.axis_index("ep") // inner
    groups = [[o * inner + i for i in range(inner)] for o in range(outer)]

    def far(step):
        return [(i, (i // inner ^ step) * inner + i % inner) for i in range(ep_count)]

    def exchange(rows):
        return lax.all_to_all(
            rows.reshape(inner, capacity, width),
            "ep",
            split_axis=0,
            concat_axis=0,
            axis_index_groups=groups,
            tiled=True,
        ).reshape(inner * capacity, width)

    marks = jnp.concatenate([routes, gate_levels], axis=1).astype(BF16)
    marks = jnp.pad(marks, ((0, 0), (0, LANES - 2 * top_count)))
    own = jnp.concatenate([tokens, marks], axis=1)
    blocks = [own] + [lax.ppermute(own, "ep", far(k)) for k in range(1, outer)]

    below = jnp.tril(jnp.ones((tok_rows, tok_rows), BF16), -1)
    experts = (plane * inner + jnp.arange(inner)).astype(F32)
    slots = jnp.arange(capacity, dtype=F32)

    def tables(block):
        ids = block[:, width : width + top_count].astype(F32)
        levels = block[:, width + top_count : width + 2 * top_count].astype(F32)
        hit = ids[:, :, None] == experts[None, None, :]
        named = jnp.any(hit, axis=1)
        slot = jnp.dot(below, named.astype(BF16), preferred_element_type=F32)
        slot = jnp.where(named, slot, -1.0)
        share = levels / jnp.sum(levels, axis=1, keepdims=True)
        share = jnp.sum(jnp.where(hit, share[:, :, None], 0.0), axis=1)
        match = slot[:, :, None] == slots[None, None, :]
        pick = match.astype(BF16).reshape(tok_rows, inner * capacity)
        mix = jnp.where(match, share[:, :, None], 0.0).astype(BF16)
        return pick, mix.reshape(tok_rows, inner * capacity)

    mixes, arrived = [], []
    for block in blocks:
        pick, mix = tables(block)
        packed = lax.dot_general(
            pick, block[:, :width], (((0,), (0,)), ((), ())), preferred_element_type=F32
        ).astype(BF16)
        mixes.append(mix)
        arrived.append(exchange(packed))

    parts = []
    for k in list(range(1, outer)) + [0]:
        produced = expert(arrived[k], w_gate[0], w_up[0], w_down[0])
        returned = exchange(produced)
        part = jnp.dot(mixes[k], returned, preferred_element_type=F32)
        if k:
            part = lax.ppermute(part.astype(BF16), "ep", far(k)).astype(F32)
        parts.append(part)
    total = parts[-1]
    for part in parts[:-1]:
        total = total + part
    return total.astype(BF16)


def solution(mesh):
    in_specs = (
        P("ep", "tp"),
        P("ep", None),
        P("ep", None),
        P("ep", "tp", None),
        P("ep", "tp", None),
        P("ep", None, "tp"),
    )
    return jax.shard_map(
        on_device, mesh=mesh, in_specs=in_specs, out_specs=P("ep", "tp"), check_vma=False
    )
```

```python
import jax
import jax.numpy as jnp
from jax import lax
from jax.experimental import pallas as pl
from jax.experimental.pallas import tpu as pltpu
from jax.sharding import PartitionSpec as P

F32 = jnp.float32
BF16 = jnp.bfloat16
LANES = 128
MIB = 1 << 20


def vmem(count):
    return [pl.BlockSpec(memory_space=pltpu.VMEM)] * count


def smem():
    return pl.BlockSpec(memory_space=pltpu.SMEM)


def params(limit):
    return pltpu.CompilerParams(vmem_limit_bytes=limit * MIB)


def cost(flops, moved):
    return pl.CostEstimate(flops=flops, bytes_accessed=moved, transcendentals=0)


def inner_size(count):
    size = 1
    while size * size < count and count % (2 * size) == 0:
        size *= 2
    return size


def pack(block, experts, width, top, capacity):
    tok_rows = block.shape[0]
    inner = experts.shape[0]
    span = -(-capacity // LANES) * LANES

    def body(experts_ref, block_ref, mix_ref, *out_refs):
        marks = block_ref[:, width:].astype(F32)
        lane = lax.broadcasted_iota(jnp.int32, marks.shape, 1)
        levels = pltpu.roll(marks, marks.shape[1] - top, 1)
        inside = lane < top
        total = jnp.sum(jnp.where(inside, levels, 0.0), axis=1, keepdims=True)
        named, share = [], []
        gathered = jnp.zeros(marks.shape, F32)
        for j in range(inner):
            hit = inside & (marks == experts_ref[j].astype(F32))
            found = jnp.sum(jnp.where(hit, 1.0, 0.0), axis=1, keepdims=True)
            named.append(found)
            share.append(jnp.sum(jnp.where(hit, levels, 0.0), axis=1, keepdims=True) / total)
            gathered = jnp.where(lane == j, found, gathered)
        row = lax.broadcasted_iota(jnp.int32, (tok_rows, tok_rows), 0)
        col = lax.broadcasted_iota(jnp.int32, (tok_rows, tok_rows), 1)
        below = jnp.where(col < row, 1.0, 0.0).astype(BF16)
        slots = jnp.dot(below, gathered.astype(BF16), preferred_element_type=F32)
        place = lax.broadcasted_iota(jnp.int32, (tok_rows, span), 1).astype(F32)
        data = block_ref[:, :width]
        for j in range(inner):
            match = (place == slots[:, j : j + 1]) & (named[j] > 0.0)
            mix_ref[:, j * span : (j + 1) * span] = jnp.where(match, share[j], 0.0).astype(BF16)
            pick = jnp.where(match, 1.0, 0.0).astype(BF16)
            rows = lax.dot_general(
                pick, data, (((0,), (0,)), ((), ())), preferred_element_type=F32
            )
            out_refs[j][...] = rows[:capacity].astype(BF16)

    out = pl.pallas_call(
        body,
        out_shape=[jax.ShapeDtypeStruct((tok_rows, inner * span), BF16)]
        + [jax.ShapeDtypeStruct((capacity, width), BF16)] * inner,
        in_specs=[smem()] + vmem(1),
        out_specs=vmem(1 + inner),
        compiler_params=params(8),
        cost_estimate=cost(2 * inner * span * tok_rows * width, 2 * 3 * tok_rows * width),
        name="pack",
    )(experts, block)
    return out[0], list(out[1:])


def lift(rows, w_gate, w_up, side):
    capacity, width = rows[0].shape
    count = len(rows)
    half = w_gate.shape[1] // 2
    total = count * capacity

    def body(side_ref, *refs):
        in_refs, (gate_ref, up_ref, give_ref, keep_ref, held) = refs[:count], refs[count:]
        for j in range(count):
            held[j * capacity : (j + 1) * capacity, :] = in_refs[j][...]
        mine = pl.multiple_of(side_ref[0] * half, LANES)
        theirs = pl.multiple_of((1 - side_ref[0]) * half, LANES)
        data = held[...]
        for at, w_ref in ((0, gate_ref), (half, up_ref)):
            give_ref[:, at : at + half] = jnp.dot(
                data, w_ref[:, pl.ds(theirs, half)], preferred_element_type=F32
            ).astype(BF16)
        for at, w_ref in ((0, gate_ref), (half, up_ref)):
            keep_ref[:, at : at + half] = jnp.dot(
                data, w_ref[:, pl.ds(mine, half)], preferred_element_type=F32
            )

    return pl.pallas_call(
        body,
        out_shape=[
            jax.ShapeDtypeStruct((total, 2 * half), BF16),
            jax.ShapeDtypeStruct((total, 2 * half), F32),
        ],
        in_specs=[smem()] + vmem(count + 2),
        out_specs=vmem(2),
        scratch_shapes=[pltpu.VMEM((total, width), BF16)],
        compiler_params=params(24),
        cost_estimate=cost(8 * total * width * half, 8 * width * half),
        name="lift",
    )(side, *rows, w_gate, w_up)


def activate(keep, got):
    total, wide = keep.shape
    half = wide // 2

    def body(keep_ref, got_ref, out_ref):
        gate = keep_ref[:, :half] + got_ref[:, :half].astype(F32)
        up = keep_ref[:, half:] + got_ref[:, half:].astype(F32)
        out_ref[...] = (gate / (1.0 + jnp.exp(-gate)) * up).astype(BF16)

    return pl.pallas_call(
        body,
        out_shape=jax.ShapeDtypeStruct((total, half), BF16),
        in_specs=vmem(2),
        out_specs=vmem(1)[0],
        compiler_params=params(8),
        cost_estimate=cost(20 * total * half, 8 * total * half),
        name="activate",
    )(keep, got)


def lower(own, other, w_down, side, count):
    total, half = own.shape
    width = w_down.shape[1]
    capacity = total // count

    def body(side_ref, own_ref, other_ref, w_ref, *out_refs):
        mine = pl.multiple_of(side_ref[0] * half, LANES)
        theirs = pl.multiple_of((1 - side_ref[0]) * half, LANES)
        out = jnp.dot(own_ref[...], w_ref[pl.ds(mine, half), :], preferred_element_type=F32)
        out = out + jnp.dot(
            other_ref[...], w_ref[pl.ds(theirs, half), :], preferred_element_type=F32
        )
        for j in range(count):
            out_refs[j][...] = out[j * capacity : (j + 1) * capacity].astype(BF16)

    return pl.pallas_call(
        body,
        out_shape=[jax.ShapeDtypeStruct((capacity, width), BF16)] * count,
        in_specs=[smem()] + vmem(3),
        out_specs=vmem(count),
        compiler_params=params(16),
        cost_estimate=cost(4 * total * half * width, 4 * half * width),
        name="lower",
    )(side, own, other, w_down)


def expert(rows, w_gate, w_up, w_down):
    if lax.axis_size("tp") == 2:
        pairs = [(0, 1), (1, 0)]
        side = lax.axis_index("tp").reshape(1).astype(jnp.int32)
        give, keep = lift(rows, w_gate, w_up, side)
        hidden = activate(keep, lax.ppermute(give, "tp", pairs))
        return lower(hidden, lax.ppermute(hidden, "tp", pairs), w_down, side, len(rows))
    data = jnp.concatenate(rows, axis=0)
    gate_part = jnp.dot(data, w_gate, preferred_element_type=F32)
    up_part = jnp.dot(data, w_up, preferred_element_type=F32)
    gate_sum = lax.psum_scatter(gate_part, "tp", scatter_dimension=1, tiled=True)
    up_sum = lax.psum_scatter(up_part, "tp", scatter_dimension=1, tiled=True)
    hidden = (jax.nn.silu(gate_sum) * up_sum).astype(BF16)
    hidden = lax.all_gather(hidden, "tp", axis=1, tiled=True)
    out = jnp.dot(hidden, w_down, preferred_element_type=F32).astype(BF16)
    return jnp.split(out, len(rows), axis=0)


def combine(rows, mix, partials, out_type):
    capacity, width = rows[0].shape
    count = len(rows)
    tok_rows = mix.shape[0]
    span = mix.shape[1] // count

    def body(mix_ref, *refs):
        total = None
        for j in range(count):
            term = jnp.dot(
                mix_ref[:, j * span : j * span + capacity],
                refs[j][...],
                preferred_element_type=F32,
            )
            total = term if total is None else total + term
        for ref in refs[count:-1]:
            total = total + ref[...].astype(F32)
        refs[-1][...] = total.astype(out_type)

    return pl.pallas_call(
        body,
        out_shape=jax.ShapeDtypeStruct((tok_rows, width), out_type),
        in_specs=vmem(1 + count + len(partials)),
        out_specs=vmem(1)[0],
        compiler_params=params(10),
        cost_estimate=cost(2 * count * capacity * tok_rows * width, 2 * tok_rows * width),
        name="combine",
    )(mix, *rows, *partials)


def on_device(tokens, routes, gate_levels, w_gate, w_up, w_down):
    ep_count = lax.axis_size("ep")
    tok_rows, top_count = routes.shape
    assert w_gate.shape[0] == 1
    capacity = min(tok_rows, max(2, 9 * tok_rows * top_count // (8 * ep_count)))
    width = tokens.shape[1]
    inner = inner_size(ep_count)
    outer = ep_count // inner
    index = lax.axis_index("ep")
    plane, spot = index // inner, index % inner

    def move(value, hops):
        pairs = [
            (a * inner + i, b * inner + i) for a, b in hops for i in range(inner)
        ]
        return lax.ppermute(value, "ep", pairs)

    def flip(step):
        return [(a, a ^ step) for a in range(outer)]

    def near(rows):
        return [rows[0]] + [
            lax.ppermute(rows[j], "ep", [(i, i ^ j) for i in range(ep_count)])
            for j in range(1, inner)
        ]

    marks = jnp.concatenate([routes, gate_levels], axis=1).astype(BF16)
    marks = jnp.pad(marks, ((0, 0), (0, LANES - 2 * top_count)))
    own = jnp.concatenate([tokens, marks], axis=1)
    if outer == 4:
        middle = (plane == 1) | (plane == 2)
        side = move(own, flip(1))
        across = move(own, [(1, 2), (2, 1)])
        outward = move(across, [(1, 0), (2, 3)])
        relayed = move(side, [(1, 2), (2, 1)])
        last = move(relayed, [(1, 0), (2, 3)])
        blocks = [own, side, jnp.where(middle, relayed, outward), jnp.where(middle, across, last)]
    else:
        blocks = [own] + [move(own, flip(k)) for k in range(1, outer)]

    experts = (plane * inner + (spot ^ jnp.arange(inner))).astype(jnp.int32)
    mixes, arrived = [], []
    for block in blocks:
        mix, packed = pack(block, experts, width, top_count, capacity)
        mixes.append(mix)
        arrived.append(near(packed))

    partials = []
    for k in list(range(2, outer)) + [1]:
        returned = near(expert(arrived[k], w_gate[0], w_up[0], w_down[0]))
        partials.append(move(combine(returned, mixes[k], [], BF16), flip(k)))
    returned = near(expert(arrived[0], w_gate[0], w_up[0], w_down[0]))
    return combine(returned, mixes[0], partials, BF16)


def solution(mesh):
    in_specs = (
        P("ep", "tp"),
        P("ep", None),
        P("ep", None),
        P("ep", "tp", None),
        P("ep", "tp", None),
        P("ep", None, "tp"),
    )
    return jax.shard_map(
        on_device, mesh=mesh, in_specs=in_specs, out_specs=P("ep", "tp"), check_vma=False
    )
```

```python
import jax
import jax.numpy as jnp
from jax import lax
from jax.experimental import pallas as pl
from jax.experimental.pallas import tpu as pltpu
from jax.sharding import PartitionSpec as P


F32 = jnp.float32
BF16 = jnp.bfloat16
LANES = 128
MIB = 1 << 20
PIECES = 4


def vmem(count):
    return [pl.BlockSpec(memory_space=pltpu.VMEM)] * count


def hbm(count):
    return [pl.BlockSpec(memory_space=pltpu.HBM)] * count


def from_hbm(value):
    return pltpu.with_memory_space_constraint(value, pltpu.HBM)


def params(limit):
    return pltpu.CompilerParams(vmem_limit_bytes=limit * MIB)


def cost(flops, moved):
    return pl.CostEstimate(flops=flops, bytes_accessed=moved, transcendentals=0)


def inner_size(count):
    size = 1
    while size * size < count and count % (2 * size) == 0:
        size *= 2
    return size


def load(value):
    rows = value.shape[0] // PIECES

    def body(src_ref, dst_ref, sems):
        copies = [
            pltpu.make_async_copy(
                src_ref.at[pl.ds(p * rows, rows)], dst_ref.at[pl.ds(p * rows, rows)], sems.at[p]
            )
            for p in range(PIECES)
        ]
        for copy in copies:
            copy.start()
        for copy in copies:
            copy.wait()

    return pl.pallas_call(
        body,
        out_shape=pltpu.VMEM(value.shape, value.dtype),
        in_specs=hbm(1),
        out_specs=vmem(1)[0],
        scratch_shapes=[pltpu.SemaphoreType.DMA((PIECES,))],
        compiler_params=params(2),
        name="load",
    )(from_hbm(value))


def stage(tokens, routes, gate_levels):
    tok_rows, width = tokens.shape
    top = routes.shape[1]
    direct = width % LANES == 0

    def body(routes_ref, levels_ref, tokens_ref, out_ref, held, small, sems):
        target = out_ref.at[:, :width] if direct else held
        copies = [
            pltpu.make_async_copy(routes_ref, small.at[0], sems.at[0]),
            pltpu.make_async_copy(levels_ref, small.at[1], sems.at[1]),
            pltpu.make_async_copy(tokens_ref, target, sems.at[2]),
        ]
        for copy in copies:
            copy.start()
        lane = lax.broadcasted_iota(jnp.int32, (top, LANES), 1)
        choice = lax.broadcasted_iota(jnp.int32, (top, LANES), 0)
        marks = jnp.zeros((tok_rows, LANES), F32)
        for i in range(2):
            copies[i].wait()
            spread = jnp.where(lane == choice + i * top, 1.0, 0.0).astype(BF16)
            marks = marks + lax.dot_general(
                small[i].astype(F32).astype(BF16),
                spread,
                (((0,), (0,)), ((), ())),
                preferred_element_type=F32,
            )
        out_ref[:, width:] = marks.astype(BF16)
        copies[2].wait()
        if not direct:
            out_ref[:, :width] = held[...]

    return pl.pallas_call(
        body,
        out_shape=jax.ShapeDtypeStruct((tok_rows, width + LANES), BF16),
        in_specs=hbm(3),
        out_specs=vmem(1)[0],
        scratch_shapes=[
            pltpu.VMEM((8, LANES) if direct else (tok_rows, width), BF16),
            pltpu.VMEM((2, top, tok_rows), jnp.int32),
            pltpu.SemaphoreType.DMA((3,)),
        ],
        compiler_params=params(8),
        name="stage",
    )(from_hbm(routes.T), from_hbm(gate_levels.T), from_hbm(tokens))


def pack(blocks, width, top, capacity, inner, outer):
    tok_rows = blocks[0].shape[0]
    span = -(-capacity // LANES) * LANES
    count = len(blocks)

    def body(*refs):
        block_refs, mix_ref, out_refs = refs[:count], refs[count], refs[count + 1 :]
        index = lax.axis_index("ep")
        plane, spot = index // inner, index % inner
        block = block_refs[0][...]
        if count == 2:
            middle = (plane > 0) & (plane < outer - 1)
            block = jnp.where(middle, block, block_refs[1][...])
        marks = block[:, width:].astype(F32)
        lane = lax.broadcasted_iota(jnp.int32, marks.shape, 1)
        levels = pltpu.roll(marks, marks.shape[1] - top, 1)
        inside = lane < top
        total = jnp.sum(jnp.where(inside, levels, 0.0), axis=1, keepdims=True)
        named, share = [], []
        gathered = jnp.zeros(marks.shape, F32)
        for j in range(inner):
            hit = inside & (marks == (plane * inner + (spot ^ j)).astype(F32))
            found = jnp.sum(jnp.where(hit, 1.0, 0.0), axis=1, keepdims=True)
            named.append(found)
            share.append(jnp.sum(jnp.where(hit, levels, 0.0), axis=1, keepdims=True) / total)
            gathered = jnp.where(lane == j, found, gathered)
        row = lax.broadcasted_iota(jnp.int32, (tok_rows, tok_rows), 0)
        col = lax.broadcasted_iota(jnp.int32, (tok_rows, tok_rows), 1)
        below = jnp.where(col < row, 1.0, 0.0).astype(BF16)
        slots = jnp.dot(below, gathered.astype(BF16), preferred_element_type=F32)
        place = lax.broadcasted_iota(jnp.int32, (tok_rows, span), 1).astype(F32)
        data = block[:, :width]
        for j in range(inner):
            match = (place == slots[:, j : j + 1]) & (named[j] > 0.0)
            mix_ref[:, j * span : (j + 1) * span] = jnp.where(match, share[j], 0.0).astype(BF16)
            pick = jnp.where(match, 1.0, 0.0).astype(BF16)
            rows = lax.dot_general(
                pick, data, (((0,), (0,)), ((), ())), preferred_element_type=F32
            )
            out_refs[j][...] = rows[:capacity].astype(BF16)

    out = pl.pallas_call(
        body,
        out_shape=[jax.ShapeDtypeStruct((tok_rows, inner * span), BF16)]
        + [jax.ShapeDtypeStruct((capacity, width), BF16)] * inner,
        in_specs=vmem(count),
        out_specs=vmem(1 + inner),
        compiler_params=params(8),
        cost_estimate=cost(2 * inner * span * tok_rows * width, 2 * 3 * tok_rows * width),
        name="pack",
    )(*blocks)
    return out[0], list(out[1:])


def lift(rows, w_gate, w_up, away):
    capacity, width = rows[0].shape
    count = len(rows)
    half = w_gate.shape[1] // 2
    total = count * capacity
    kind = BF16 if away else F32

    def body(*refs):
        in_refs, (gate_ref, up_ref, out_ref, held) = refs[:count], refs[count:]
        for j in range(count):
            held[j * capacity : (j + 1) * capacity, :] = in_refs[j][...]
        side = lax.axis_index("tp")
        at = pl.multiple_of((1 - side if away else side) * half, LANES)
        data = held[...]
        for i, w_ref in enumerate((gate_ref, up_ref)):
            out_ref[:, i * half : (i + 1) * half] = jnp.dot(
                data, w_ref[:, pl.ds(at, half)], preferred_element_type=F32
            ).astype(kind)

    return pl.pallas_call(
        body,
        out_shape=jax.ShapeDtypeStruct((total, 2 * half), kind),
        in_specs=vmem(count + 2),
        out_specs=vmem(1)[0],
        scratch_shapes=[pltpu.VMEM((total, width), BF16)],
        compiler_params=params(8),
        cost_estimate=cost(4 * total * width * half, 4 * width * half),
        name="lift",
    )(*rows, w_gate, w_up)


def activate(keep, got):
    total, wide = keep.shape
    half = wide // 2

    def body(keep_ref, got_ref, out_ref):
        gate = keep_ref[:, :half] + got_ref[:, :half].astype(F32)
        up = keep_ref[:, half:] + got_ref[:, half:].astype(F32)
        out_ref[...] = (gate / (1.0 + jnp.exp(-gate)) * up).astype(BF16)

    return pl.pallas_call(
        body,
        out_shape=jax.ShapeDtypeStruct((total, half), BF16),
        in_specs=vmem(2),
        out_specs=vmem(1)[0],
        compiler_params=params(8),
        cost_estimate=cost(20 * total * half, 8 * total * half),
        name="activate",
    )(keep, got)


def lower(own, other, w_down, count):
    total, half = own.shape
    width = w_down.shape[1]
    capacity = total // count

    def body(own_ref, other_ref, w_ref, *out_refs):
        side = lax.axis_index("tp")
        mine = pl.multiple_of(side * half, LANES)
        theirs = pl.multiple_of((1 - side) * half, LANES)
        out = jnp.dot(own_ref[...], w_ref[pl.ds(mine, half), :], preferred_element_type=F32)
        out = out + jnp.dot(
            other_ref[...], w_ref[pl.ds(theirs, half), :], preferred_element_type=F32
        )
        for j in range(count):
            out_refs[j][...] = out[j * capacity : (j + 1) * capacity].astype(BF16)

    return pl.pallas_call(
        body,
        out_shape=[jax.ShapeDtypeStruct((capacity, width), BF16)] * count,
        in_specs=vmem(3),
        out_specs=vmem(count),
        compiler_params=params(16),
        cost_estimate=cost(4 * total * half * width, 4 * half * width),
        name="lower",
    )(own, other, w_down)


def combine(rows, mix, partials, out_type):
    capacity, width = rows[0].shape
    count = len(rows)
    tok_rows = mix.shape[0]
    span = mix.shape[1] // count

    def body(mix_ref, *refs):
        total = None
        for j in range(count):
            term = jnp.dot(
                mix_ref[:, j * span : j * span + capacity],
                refs[j][...],
                preferred_element_type=F32,
            )
            total = term if total is None else total + term
        for ref in refs[count:-1]:
            total = total + ref[...].astype(F32)
        refs[-1][...] = total.astype(out_type)

    return pl.pallas_call(
        body,
        out_shape=jax.ShapeDtypeStruct((tok_rows, width), out_type),
        in_specs=vmem(1 + count + len(partials)),
        out_specs=vmem(1)[0],
        compiler_params=params(10),
        cost_estimate=cost(2 * count * capacity * tok_rows * width, 2 * tok_rows * width),
        name="combine",
    )(mix, *rows, *partials)


def on_device(tokens, routes, gate_levels, w_gate, w_up, w_down):
    ep_count, tp_count = lax.axis_size("ep"), lax.axis_size("tp")
    tok_rows, top_count = routes.shape
    assert w_gate.shape[0] == 1
    w_gate, w_up, w_down = w_gate[0], w_up[0], w_down[0]
    capacity = min(tok_rows, max(2, 9 * tok_rows * top_count // (8 * ep_count)))
    width = tokens.shape[1]
    inner = inner_size(ep_count)
    outer = ep_count // inner

    def hop(value, hops):
        pairs = [(a * inner + i, b * inner + i) for a, b in hops for i in range(inner)]
        return lax.ppermute(value, "ep", pairs)

    def flip(value, step):
        pairs = [(i, (i // inner ^ step) * inner + i % inner) for i in range(ep_count)]
        return lax.ppermute(value, "ep", pairs)

    def near(rows):
        out = [rows[0]]
        for j in range(1, inner):
            out.append(lax.ppermute(rows[j], "ep", [(i, i ^ j) for i in range(ep_count)]))
        return out

    def swap(value):
        return lax.ppermute(value, "tp", [(0, 1), (1, 0)])

    def send(blocks):
        mix, packed = pack(blocks, width, top_count, capacity, inner, outer)
        return mix, near(packed)

    def expert(rows, w_gate, w_up, w_down):
        if tp_count == 2:
            give = lift(rows, w_gate, w_up, True)
            got = swap(give)
            keep = lift(rows, w_gate, w_up, False)
            hidden = activate(keep, got)
            other = swap(hidden)
            return lower(hidden, other, w_down, inner)
        data = jnp.concatenate(rows, axis=0)
        gate_part = jnp.dot(data, w_gate, preferred_element_type=F32)
        up_part = jnp.dot(data, w_up, preferred_element_type=F32)
        gate_sum = lax.psum_scatter(gate_part, "tp", scatter_dimension=1, tiled=True)
        up_sum = lax.psum_scatter(up_part, "tp", scatter_dimension=1, tiled=True)
        hidden = (jax.nn.silu(gate_sum) * up_sum).astype(BF16)
        hidden = lax.all_gather(hidden, "tp", axis=1, tiled=True)
        out = jnp.dot(hidden, w_down, preferred_element_type=F32).astype(BF16)
        return jnp.split(out, inner, axis=0)

    def gather(rows, mix, partials, kind=BF16):
        returned = near(rows)
        return combine(returned, mix, partials, kind)

    own = stage(tokens, routes, gate_levels)
    if outer != 4:
        sent = [send([own])]
        sent += [send([flip(own, k)]) for k in range(1, outer)]
        partials = []
        for k in range(1, outer):
            mix, rows = sent[k]
            part = gather(expert(rows, w_gate, w_up, w_down), mix, [])
            partials.append(flip(part, k))
        mix, rows = sent[0]
        return gather(expert(rows, w_gate, w_up, w_down), mix, partials)

    beside = flip(own, 1)
    across = hop(own, [(1, 2), (2, 1)])
    mix0, rows0 = send([own])
    relayed = hop(beside, [(1, 2), (2, 1)])
    outward = hop(across, [(1, 0), (2, 3)])
    mix1, rows1 = send([beside])
    last = hop(relayed, [(1, 0), (2, 3)])
    mix2, rows2 = send([relayed, outward])
    mix3, rows3 = send([across, last])
    weights = [load(w_gate), load(w_up), load(w_down)]
    made = [expert(rows, *weights) for rows in (rows0, rows1, rows2, rows3)]
    passed = flip(gather(made[2], mix2, []), 1)
    distant = flip(gather(made[3], mix3, [passed]), 3)
    close = flip(gather(made[1], mix1, []), 1)
    return gather(made[0], mix0, [close, distant])


def solution(mesh):
    in_specs = (
        P("ep", "tp"),
        P("ep", None),
        P("ep", None),
        P("ep", "tp", None),
        P("ep", "tp", None),
        P("ep", None, "tp"),
    )
    return jax.shard_map(
        on_device, mesh=mesh, in_specs=in_specs, out_specs=P("ep", "tp"), check_vma=False
    )
```

```python
import jax
import jax.numpy as jnp
from jax import lax
from jax.experimental import pallas as pl
from jax.experimental.pallas import tpu as pltpu
from jax.sharding import PartitionSpec as P


F32 = jnp.float32
BF16 = jnp.bfloat16
LANES = 128
MIB = 1 << 20
PIECES = 4


def vmem(count):
    return [pl.BlockSpec(memory_space=pltpu.VMEM)] * count


def hbm(count):
    return [pl.BlockSpec(memory_space=pltpu.HBM)] * count


def from_hbm(value):
    return pltpu.with_memory_space_constraint(value, pltpu.HBM)


def params(limit):
    return pltpu.CompilerParams(vmem_limit_bytes=limit * MIB)


def cost(flops, moved):
    return pl.CostEstimate(flops=flops, bytes_accessed=moved, transcendentals=0)


def inner_size(count):
    size = 1
    while size * size < count and count % (2 * size) == 0:
        size *= 2
    return size


def load(value):
    rows = value.shape[0] // PIECES

    def body(src_ref, dst_ref, sems):
        copies = [
            pltpu.make_async_copy(
                src_ref.at[pl.ds(p * rows, rows)], dst_ref.at[pl.ds(p * rows, rows)], sems.at[p]
            )
            for p in range(PIECES)
        ]
        for copy in copies:
            copy.start()
        for copy in copies:
            copy.wait()

    return pl.pallas_call(
        body,
        out_shape=pltpu.VMEM(value.shape, value.dtype),
        in_specs=hbm(1),
        out_specs=vmem(1)[0],
        scratch_shapes=[pltpu.SemaphoreType.DMA((PIECES,))],
        compiler_params=params(2),
        name="load",
    )(from_hbm(value))


def stage(tokens, routes, gate_levels):
    tok_rows, width = tokens.shape
    top = routes.shape[1]
    assert tok_rows == LANES
    tall = -(-width // LANES) * LANES
    total = tall + 2 * top

    def body(routes_ref, levels_ref, tokens_ref, out_ref, held, small, sems):
        copies = [
            pltpu.make_async_copy(tokens_ref, held, sems.at[2]),
            pltpu.make_async_copy(routes_ref, small.at[0], sems.at[0]),
            pltpu.make_async_copy(levels_ref, small.at[1], sems.at[1]),
        ]
        for copy in copies:
            copy.start()
        for copy in copies:
            copy.wait()
        for at in range(0, width, LANES):
            wide = min(LANES, width - at)
            out_ref[at : at + LANES, :wide] = held[:, at : at + wide]
        marks = jnp.concatenate([small[0], small[1]], axis=0).astype(F32)
        out_ref[tall:, :] = marks.astype(BF16)

    return pl.pallas_call(
        body,
        out_shape=jax.ShapeDtypeStruct((total, LANES), BF16),
        in_specs=hbm(3),
        out_specs=vmem(1)[0],
        scratch_shapes=[
            pltpu.VMEM((tok_rows, width), BF16),
            pltpu.VMEM((2, top, tok_rows), jnp.int32),
            pltpu.SemaphoreType.DMA((3,)),
        ],
        compiler_params=params(8),
        name="stage",
    )(from_hbm(routes.T), from_hbm(gate_levels.T), from_hbm(tokens))


def pack(blocks, width, top, capacity, inner, outer):
    tok_rows = LANES
    tall = -(-width // LANES) * LANES
    span = -(-capacity // LANES) * LANES
    count = len(blocks)

    def body(*refs):
        block_refs, mix_ref, out_refs = refs[:count], refs[count], refs[count + 1 :]
        index = lax.axis_index("ep")
        plane, spot = index // inner, index % inner
        block = block_refs[0][...]
        if count == 2:
            middle = (plane > 0) & (plane < outer - 1)
            block = jnp.where(middle, block, block_refs[1][...])
        choice = lax.broadcasted_iota(jnp.int32, (2 * top, LANES), 0)
        spread = lax.broadcasted_iota(jnp.int32, (2 * top, LANES), 1) == choice
        marks = lax.dot_general(
            block[tall:],
            jnp.where(spread, 1.0, 0.0).astype(BF16),
            (((0,), (0,)), ((), ())),
            preferred_element_type=F32,
        )
        lane = lax.broadcasted_iota(jnp.int32, marks.shape, 1)
        levels = pltpu.roll(marks, marks.shape[1] - top, 1)
        inside = lane < top
        total = jnp.sum(jnp.where(inside, levels, 0.0), axis=1, keepdims=True)
        named, share = [], []
        gathered = jnp.zeros(marks.shape, F32)
        for j in range(inner):
            hit = inside & (marks == (plane * inner + (spot ^ j)).astype(F32))
            found = jnp.sum(jnp.where(hit, 1.0, 0.0), axis=1, keepdims=True)
            named.append(found)
            share.append(jnp.sum(jnp.where(hit, levels, 0.0), axis=1, keepdims=True) / total)
            gathered = jnp.where(lane == j, found, gathered)
        row = lax.broadcasted_iota(jnp.int32, (tok_rows, tok_rows), 0)
        col = lax.broadcasted_iota(jnp.int32, (tok_rows, tok_rows), 1)
        below = jnp.where(col < row, 1.0, 0.0).astype(BF16)
        slots = jnp.dot(below, gathered.astype(BF16), preferred_element_type=F32)
        place = lax.broadcasted_iota(jnp.int32, (tok_rows, span), 1).astype(F32)
        data = jnp.concatenate(
            [
                block[at : at + LANES, : min(LANES, width - at)]
                for at in range(0, width, LANES)
            ],
            axis=1,
        )
        for j in range(inner):
            match = (place == slots[:, j : j + 1]) & (named[j] > 0.0)
            mix_ref[:, j * span : (j + 1) * span] = jnp.where(match, share[j], 0.0).astype(BF16)
            pick = jnp.where(match, 1.0, 0.0).astype(BF16)
            rows = lax.dot_general(
                pick[:, :capacity], data, (((0,), (0,)), ((), ())), preferred_element_type=F32
            )
            out_refs[j][...] = rows.astype(BF16)

    out = pl.pallas_call(
        body,
        out_shape=[jax.ShapeDtypeStruct((tok_rows, inner * span), BF16)]
        + [jax.ShapeDtypeStruct((capacity, width), BF16)] * inner,
        in_specs=vmem(count),
        out_specs=vmem(1 + inner),
        compiler_params=params(8),
        cost_estimate=cost(2 * inner * span * tok_rows * width, 2 * 3 * tok_rows * width),
        name="pack",
    )(*blocks)
    return out[0], list(out[1:])


def lift(rows, w_gate, w_up, away):
    capacity, width = rows[0].shape
    count = len(rows)
    half = w_gate.shape[1] // 2
    total = count * capacity
    kind = BF16 if away else F32

    def body(*refs):
        in_refs, (gate_ref, up_ref, out_ref, held) = refs[:count], refs[count:]
        for j in range(count):
            held[j * capacity : (j + 1) * capacity, :] = in_refs[j][...]
        side = lax.axis_index("tp")
        at = pl.multiple_of((1 - side if away else side) * half, LANES)
        data = held[...]
        for i, w_ref in enumerate((gate_ref, up_ref)):
            out_ref[:, i * half : (i + 1) * half] = jnp.dot(
                data, w_ref[:, pl.ds(at, half)], preferred_element_type=F32
            ).astype(kind)

    return pl.pallas_call(
        body,
        out_shape=jax.ShapeDtypeStruct((total, 2 * half), kind),
        in_specs=vmem(count + 2),
        out_specs=vmem(1)[0],
        scratch_shapes=[pltpu.VMEM((total, width), BF16)],
        compiler_params=params(8),
        cost_estimate=cost(4 * total * width * half, 4 * width * half),
        name="lift",
    )(*rows, w_gate, w_up)


def activate(keep, got):
    total, wide = keep.shape
    half = wide // 2

    def body(keep_ref, got_ref, out_ref):
        gate = keep_ref[:, :half] + got_ref[:, :half].astype(F32)
        up = keep_ref[:, half:] + got_ref[:, half:].astype(F32)
        out_ref[...] = (gate / (1.0 + jnp.exp(-gate)) * up).astype(BF16)

    return pl.pallas_call(
        body,
        out_shape=jax.ShapeDtypeStruct((total, half), BF16),
        in_specs=vmem(2),
        out_specs=vmem(1)[0],
        compiler_params=params(8),
        cost_estimate=cost(20 * total * half, 8 * total * half),
        name="activate",
    )(keep, got)


def lower(own, other, w_down, count):
    total, half = own.shape
    width = w_down.shape[1]
    capacity = total // count

    def body(own_ref, other_ref, w_ref, *out_refs):
        side = lax.axis_index("tp")
        mine = pl.multiple_of(side * half, LANES)
        theirs = pl.multiple_of((1 - side) * half, LANES)
        out = jnp.dot(own_ref[...], w_ref[pl.ds(mine, half), :], preferred_element_type=F32)
        out = out + jnp.dot(
            other_ref[...], w_ref[pl.ds(theirs, half), :], preferred_element_type=F32
        )
        for j in range(count):
            out_refs[j][...] = out[j * capacity : (j + 1) * capacity].astype(BF16)

    return pl.pallas_call(
        body,
        out_shape=[jax.ShapeDtypeStruct((capacity, width), BF16)] * count,
        in_specs=vmem(3),
        out_specs=vmem(count),
        compiler_params=params(16),
        cost_estimate=cost(4 * total * half * width, 4 * half * width),
        name="lower",
    )(own, other, w_down)


def combine(rows, mix, partials, out_type):
    capacity, width = rows[0].shape
    count = len(rows)
    tok_rows = mix.shape[0]
    span = mix.shape[1] // count

    def body(mix_ref, *refs):
        total = None
        for j in range(count):
            term = jnp.dot(
                mix_ref[:, j * span : j * span + capacity],
                refs[j][...],
                preferred_element_type=F32,
            )
            total = term if total is None else total + term
        for ref in refs[count:-1]:
            total = total + ref[...].astype(F32)
        refs[-1][...] = total.astype(out_type)

    return pl.pallas_call(
        body,
        out_shape=jax.ShapeDtypeStruct((tok_rows, width), out_type),
        in_specs=vmem(1 + count + len(partials)),
        out_specs=vmem(1)[0],
        compiler_params=params(10),
        cost_estimate=cost(2 * count * capacity * tok_rows * width, 2 * tok_rows * width),
        name="combine",
    )(mix, *rows, *partials)


def close_sum(total, part):
    tok_rows, width = total.shape
    rows = tok_rows // PIECES

    def body(total_ref, part_ref, out_ref, held, sems):
        copies = []
        for p in range(PIECES):
            here = pl.ds(p * rows, rows)
            held[here] = (total_ref[here] + part_ref[here].astype(F32)).astype(BF16)
            copies.append(pltpu.make_async_copy(held.at[here], out_ref.at[here], sems.at[p]))
            copies[-1].start()
        for copy in copies:
            copy.wait()

    return pl.pallas_call(
        body,
        out_shape=jax.ShapeDtypeStruct((tok_rows, width), BF16),
        in_specs=vmem(2),
        out_specs=hbm(1)[0],
        scratch_shapes=[pltpu.VMEM((tok_rows, width), BF16), pltpu.SemaphoreType.DMA((PIECES,))],
        compiler_params=params(2),
        name="close",
    )(total, part)


def on_device(tokens, routes, gate_levels, w_gate, w_up, w_down):
    ep_count, tp_count = lax.axis_size("ep"), lax.axis_size("tp")
    tok_rows, top_count = routes.shape
    assert w_gate.shape[0] == 1
    w_gate, w_up, w_down = w_gate[0], w_up[0], w_down[0]
    capacity = min(tok_rows, max(2, 9 * tok_rows * top_count // (8 * ep_count)))
    width = tokens.shape[1]
    inner = inner_size(ep_count)
    outer = ep_count // inner
    ordered = outer == 4 and tp_count == 2

    def hop(value, hops):
        pairs = [(a * inner + i, b * inner + i) for a, b in hops for i in range(inner)]
        return lax.ppermute(value, "ep", pairs)

    def flip(value, step):
        pairs = [(i, (i // inner ^ step) * inner + i % inner) for i in range(ep_count)]
        return lax.ppermute(value, "ep", pairs)

    def near(rows):
        out = [rows[0]]
        for j in range(1, inner):
            out.append(lax.ppermute(rows[j], "ep", [(i, i ^ j) for i in range(ep_count)]))
        return out

    def swap(value):
        return lax.ppermute(value, "tp", [(0, 1), (1, 0)])

    def send(blocks):
        mix, packed = pack(blocks, width, top_count, capacity, inner, outer)
        return mix, near(packed)

    def expert(rows, w_gate, w_up, w_down):
        if tp_count == 2:
            give = lift(rows, w_gate, w_up, True)
            got = swap(give)
            keep = lift(rows, w_gate, w_up, False)
            hidden = activate(keep, got)
            other = swap(hidden)
            return lower(hidden, other, w_down, inner)
        data = jnp.concatenate(rows, axis=0)
        gate_part = jnp.dot(data, w_gate, preferred_element_type=F32)
        up_part = jnp.dot(data, w_up, preferred_element_type=F32)
        gate_sum = lax.psum_scatter(gate_part, "tp", scatter_dimension=1, tiled=True)
        up_sum = lax.psum_scatter(up_part, "tp", scatter_dimension=1, tiled=True)
        hidden = (jax.nn.silu(gate_sum) * up_sum).astype(BF16)
        hidden = lax.all_gather(hidden, "tp", axis=1, tiled=True)
        out = jnp.dot(hidden, w_down, preferred_element_type=F32).astype(BF16)
        return jnp.split(out, inner, axis=0)

    def gather(rows, mix, partials, kind=BF16):
        returned = near(rows)
        return combine(returned, mix, partials, kind)

    own = stage(tokens, routes, gate_levels)
    if not ordered:
        sent = [send([own])]
        sent += [send([flip(own, k)]) for k in range(1, outer)]
        partials = []
        for k in range(1, outer):
            mix, rows = sent[k]
            part = gather(expert(rows, w_gate, w_up, w_down), mix, [])
            partials.append(flip(part, k))
        mix, rows = sent[0]
        return gather(expert(rows, w_gate, w_up, w_down), mix, partials)

    swap_middle, to_ends = [(1, 2), (2, 1)], [(1, 0), (2, 3)]
    beside = flip(own, 1)
    across = hop(own, swap_middle)
    mix0, rows0 = send([own])
    relayed = hop(beside, swap_middle)
    outward = hop(across, to_ends)
    mix1, rows1 = send([beside])
    last = hop(relayed, to_ends)
    mix2, rows2 = send([relayed, outward])
    mix3, rows3 = send([across, last])
    weights = [load(w_gate), load(w_up), load(w_down)]
    made = [expert(rows, *weights) for rows in (rows0, rows1, rows2, rows3)]
    passed = flip(gather(made[2], mix2, []), 1)
    distant = flip(gather(made[3], mix3, [passed]), 3)
    close = flip(gather(made[1], mix1, []), 1)
    total = gather(made[0], mix0, [distant], F32)
    return close_sum(total, close)


def solution(mesh):
    in_specs = (
        P("ep", "tp"),
        P("ep", None),
        P("ep", None),
        P("ep", "tp", None),
        P("ep", "tp", None),
        P("ep", None, "tp"),
    )
    return jax.shard_map(
        on_device, mesh=mesh, in_specs=in_specs, out_specs=P("ep", "tp"), check_vma=False
    )
```
